32 devices in a mesh: dp: 8 (over z, x), tensor: 4 (over y, core).
Axes of the slice: x: 2, y: 2, z: 4, core: 2. Of those that a mesh axis runs over, the one named last changes fastest.
Arguments:
- tokens: bfloat16 [16384, 768], P(('dp', 'tensor')), may hold values from -6 to 6
- gain_one: float32 [768], P('dp'), may hold values from 0.5 to 1.5
- gain_two: float32 [768], P('dp'), may hold values from 0.5 to 1.5
- qkv_weight: float32 [3, 768, 768], P(None, 'dp', 'tensor'), may hold values from -0.21875 to 0.21875
- feature_weight: float32 [12, 64, 64], P('tensor', 'dp'), may hold values from -1.5 to 1.5
- out_weight: float32 [768, 768], P('tensor', 'dp'), may hold values from -1.75 to 1.75
- up_weight: float32 [768, 3072], P('dp', 'tensor'), may hold values from -0.21875 to 0.21875
- down_weight: float32 [3072, 768], P('tensor', 'dp'), may hold values from -0.109375 to 0.109375
- cotangent: bfloat16 [16384, 768], P(('dp', 'tensor')), may hold values from -6 to 6
Outputs:
- block_out: float32 [16384, 768], P(('dp', 'tensor'))
- tokens_grad: float32 [16384, 768], P(('dp', 'tensor'))
- gain_one_grad: float32 [768], P('dp')
- gain_two_grad: float32 [768], P('dp')
- qkv_weight_grad: float32 [3, 768, 768], P(None, 'dp', 'tensor')
- feature_weight_grad: float32 [12, 64, 64], P('tensor', 'dp')
- out_weight_grad: float32 [768, 768], P('tensor', 'dp')
- up_weight_grad: float32 [768, 3072], P('dp', 'tensor')
- down_weight_grad: float32 [3072, 768], P('tensor', 'dp')
The draws below stay inside these ranges and needn't reach their ends.
All inputs are finite; a program needn't handle non-finite values.
Results may differ from the reference program's by a relative error of at most 0.017.
Values may be sent and summed in bfloat16 or wider, within the bound.
A program may use at most 192 MiB of HBM per device.

```python
import jax
import jax.numpy as jnp
from jax import lax

D = 768
HEADS = 12
HD = 64
FEAT = 128
FF = 3072
GROUP = 64
SEQ = 2048
TOKENS = 16384
N_DP = 8


def with_spikes(values, rng, source, target, blocks, factor):
    def block_of(position):
        return (jnp.arange(values.shape[position]) // (values.shape[position] // blocks)).reshape((-1,) + (1,) * (values.ndim - 1 - position))

    one_side = jax.random.permutation(rng, blocks)[block_of(target)]
    other_side = (block_of(target) + blocks // 2) % blocks
    return jnp.where((block_of(source) == one_side) | (block_of(source) == other_side), factor * values, values)


def block_scale(stream_key, extent, shards, low, high):
    def one(dim, shards_of):
        draws = jax.random.uniform(jax.random.fold_in(jax.random.fold_in(stream_key, 6), dim), (shards_of,), jnp.float32, low / len(shards), high / len(shards))
        return jnp.repeat(jnp.exp(draws), extent[dim] // shards_of).reshape((-1,) + (1,) * (len(extent) - dim - 1))

    gain = one(*shards[0])
    for cut in shards[1:]:
        gain = gain * one(*cut)
    return gain


def normal_values(stream_key, dims, deviation, reach, pieces=(), dtype=jnp.bfloat16):
    values = jax.random.normal(stream_key, dims, jnp.float32) * deviation
    if len(pieces) > 0:
        values = block_scale(stream_key, dims, pieces, -0.22, 0.18) * values
    return jnp.clip(values, min=-reach, max=reach).astype(dtype)


def bell_draw_with(own_key, extent, width, reach, shards, heavy, kind=jnp.bfloat16):
    entries = width * jax.random.normal(own_key, extent, jnp.float32)
    if shards:
        entries = entries * block_scale(own_key, extent, shards, -0.22, 0.18)
    return jnp.clip(with_spikes(entries, jax.random.fold_in(own_key, 3), *heavy), -reach, reach).astype(kind)


def setup_inputs(seed: int = 0) -> dict:
    streams_of = jax.random.split(jax.random.key(seed), 10)
    return {
        "tokens": bell_draw_with(streams_of[0], (TOKENS, D), 1.0, 6.0, ((0, 32),), (0, 1, 32, 2.75)),
        "gain_one": jnp.clip(1.0 + 0.1 * jax.random.normal(streams_of[1], (D,), jnp.float32), 0.5, 1.5),
        "gain_two": jnp.clip(1.0 + 0.1 * jax.random.normal(streams_of[2], (D,), jnp.float32), 0.5, 1.5),
        "qkv_weight": normal_values(streams_of[3], (3, D, D), D ** -0.5, 0.21875, ((1, 8), (2, 4)), jnp.float32),
        "feature_weight": normal_values(streams_of[4], (HEADS, HD, HD), 0.25, 1.5, ((0, 4), (1, 8)), jnp.float32),
        "out_weight": normal_values(streams_of[5], (D, D), (D // 64) ** -0.5, 1.75, ((0, 4), (1, 8)), jnp.float32),
        "up_weight": normal_values(streams_of[6], (D, FF), D ** -0.5, 0.21875, ((0, 8), (1, 4)), jnp.float32),
        "down_weight": normal_values(streams_of[7], (FF, D), FF ** -0.5, 0.109375, ((0, 4), (1, 8)), jnp.float32),
        "cotangent": bell_draw_with(streams_of[8], (TOKENS, D), 1.0, 6.0, ((0, 32),), (0, 1, 32, 2.75)),
    }


@jax.custom_vjp
def low(v):
    return lax.optimization_barrier(v.astype(jnp.bfloat16)).astype(jnp.float32)

@jax.custom_vjp
def low_back(v):
    return v

def low_keep(v):
    return (low(v), None)

def low_pass(kept, grad):
    return (grad,)

def back_keep(v):
    return (v, None)

def back_low(kept, grad):
    return (low(grad),)
low.defvjp(low_keep, low_pass)
low_back.defvjp(back_keep, back_low)
highest = lax.Precision.HIGHEST
epsilon = 1e-05

def layer_norm(activations, gain_vector):
    center = activations - lax.optimization_barrier(jnp.mean(activations, axis=-1, keepdims=True))
    spread = lax.optimization_barrier(jnp.mean(center * center, axis=-1, keepdims=True))
    return center * lax.rsqrt(spread + epsilon) * gain_vector

def feature_map(logits):
    return jnp.concatenate([jax.nn.softmax(logits, axis=-1), jax.nn.softmax(-logits, axis=-1)], axis=-1)

def gelu_tanh(upper_part):
    return jax.nn.gelu(upper_part, approximate=True)

def causal_mask(block_size):
    row_index = lax.broadcasted_iota(jnp.int32, (block_size, block_size), 0)
    column_index = lax.broadcasted_iota(jnp.int32, (block_size, block_size), 1)
    return (column_index <= row_index).astype(jnp.float32)

def linear_attention(phi_query, phi_key, value_rows, causal):
    length = phi_query.shape[0]
    blocks = length // GROUP
    query_blocks = phi_query.reshape(blocks, GROUP, HEADS, FEAT)
    key_blocks = phi_key.reshape(blocks, GROUP, HEADS, FEAT)
    value_blocks = value_rows.reshape(blocks, GROUP, HEADS, HD)
    scores = jnp.einsum('bqhf,bkhf->bhqk', query_blocks, key_blocks, precision=highest) * causal
    scores = low_back(low(scores))
    intra_num = jnp.einsum('bhqk,bkhe->bqhe', scores, value_blocks, precision=highest)
    intra_den = jnp.transpose(lax.optimization_barrier(jnp.sum(scores, axis=-1)), (0, 2, 1))
    states = low_back(jnp.einsum('bkhf,bkhe->bhfe', key_blocks, value_blocks, precision=highest))
    prefix = low(jnp.cumsum(states, axis=0) - states)
    key_sums = lax.optimization_barrier(jnp.sum(key_blocks, axis=1))
    key_prefix = jnp.cumsum(key_sums, axis=0) - key_sums
    numerator = low_back(intra_num + jnp.einsum('bqhf,bhfe->bqhe', query_blocks, prefix, precision=highest))
    denominator = intra_den + jnp.einsum('bqhf,bhf->bqh', query_blocks, key_prefix, precision=highest)
    return (numerator / denominator[..., None]).reshape(length, HEADS * HD)

def block_forward(sequence_rows, gain_one, gain_two, qkv_weight, feature_weight, out_weight, up_weight, down_weight):
    length = sequence_rows.shape[0]
    normed = low(layer_norm(sequence_rows, low(gain_one)))
    qkv_low = low(qkv_weight)
    query_rows = low_back(jnp.dot(normed, qkv_low[0], precision=highest)).reshape(length, HEADS, HD)
    key_rows = low_back(jnp.dot(normed, qkv_low[1], precision=highest)).reshape(length, HEADS, HD)
    value_rows = low_back(low(jnp.dot(normed, qkv_low[2], precision=highest))).reshape(length, HEADS, HD)
    feature_low = low(feature_weight)
    phi_query = low(feature_map(jnp.einsum('lhd,hde->lhe', query_rows, feature_low, precision=highest)))
    phi_key = low(feature_map(jnp.einsum('lhd,hde->lhe', key_rows, feature_low, precision=highest)))
    attended = low(linear_attention(phi_query, phi_key, value_rows, causal_mask(GROUP)))
    middle = sequence_rows + low_back(jnp.dot(attended, low(out_weight), precision=highest))
    normed_two = low(layer_norm(middle, low(gain_two)))
    upper_part = low_back(jnp.dot(normed_two, low(up_weight), precision=highest))
    hidden = low(gelu_tanh(upper_part))
    return middle + low_back(jnp.dot(hidden, low(down_weight), precision=highest))

def reference(tokens, gain_one, gain_two, qkv_weight, feature_weight, out_weight, up_weight, down_weight, cotangent):
    weights = (gain_one, gain_two, qkv_weight, feature_weight, out_weight, up_weight, down_weight)
    sequence_rows = tokens.astype(jnp.float32).reshape(N_DP, SEQ, D)
    sequence_cotangents = cotangent.astype(jnp.float32).reshape(N_DP, SEQ, D)

    def one_sequence(totals, inputs_pair):
        sequence, cotangents = inputs_pair
        result, pullback = jax.vjp(block_forward, sequence, *weights)
        gradients = pullback(cotangents)
        totals = jax.tree.map(lambda running, gradient: running + gradient, totals, tuple(gradients[1:]))
        return (totals, (result, gradients[0]))
    zero_totals = jax.tree.map(jnp.zeros_like, weights)
    totals, outputs_pair = lax.scan(one_sequence, zero_totals, (sequence_rows, sequence_cotangents))
    results, input_grads = outputs_pair
    return (results.reshape(TOKENS, D), input_grads.reshape(TOKENS, D), totals[0], totals[1], totals[2], totals[3], totals[4], totals[5], totals[6])
```

```python
import functools

import jax
import jax.numpy as jnp
from jax import lax
from jax.experimental import pallas as pl
from jax.experimental.pallas import tpu as pltpu
from jax.sharding import PartitionSpec as P

bfloat = jnp.bfloat16
single = jnp.float32
EPSILON = 1e-5
HEAD = 64
FEAT = 128
LIMIT = 64000000


def mm(left, right):
    return jnp.dot(left, right, preferred_element_type=single)


def mm_tn(left, right):
    return lax.dot_general(left, right, (((0,), (0,)), ((), ())), preferred_element_type=single)


def mm_nt(left, right):
    return lax.dot_general(left, right, (((1,), (1,)), ((), ())), preferred_element_type=single)


def norm_parts(rows):
    center = rows - jnp.mean(rows, axis=-1, keepdims=True)
    spread = jnp.mean(center * center, axis=-1, keepdims=True)
    scale = lax.rsqrt(spread + EPSILON)
    return center * scale, scale


def norm_back(unit, scale, grad, gain):
    scaled = grad * gain
    return scale * (
        scaled
        - jnp.mean(scaled, axis=-1, keepdims=True)
        - unit * jnp.mean(scaled * unit, axis=-1, keepdims=True)
    )


def split_low(values):
    high = values.astype(bfloat)
    return high, (values - high.astype(single)).astype(bfloat)


def half_ones(width):
    row = lax.broadcasted_iota(jnp.int32, (width, width), 0) // HEAD
    column = lax.broadcasted_iota(jnp.int32, (width, width), 1) // HEAD
    return (row == column).astype(single).astype(bfloat)


def causal_keep(length):
    row = lax.broadcasted_iota(jnp.int32, (length, length), 0)
    column = lax.broadcasted_iota(jnp.int32, (length, length), 1)
    return column <= row


def features_kernel(x_ref, gain_ref, s_ref, f_ref, normed_ref, qk_ref, phi_ref, vx_ref, tot_ref):
    @pl.when(pl.program_id(0) == 0)
    def _():
        unit, _ = norm_parts(x_ref[...].astype(single))
        normed_ref[...] = (unit * gain_ref[...]).astype(bfloat)

    normed = normed_ref[...]
    heads = f_ref.shape[0]
    tokens = normed.shape[0]
    qk_width = heads * 2 * HEAD
    ones = half_ones(2 * FEAT)
    lane = lax.broadcasted_iota(jnp.int32, (1, HEAD), 1)
    tail = jnp.broadcast_to((lane < 2).astype(single).astype(bfloat), (tokens, HEAD))
    group = lax.broadcasted_iota(jnp.int32, (1, FEAT), 1) < HEAD
    value = mm(normed, s_ref[:, qk_width : qk_width + heads * HEAD]).astype(bfloat)
    for h in range(heads):
        pair = mm(normed, s_ref[:, h * FEAT : (h + 1) * FEAT])
        high, rest = split_low(pair)
        qk_ref[:, h * FEAT : (h + 1) * FEAT] = high
        logits = mm(high, f_ref[h]) + mm(rest, f_ref[h])
        sides = []
        for side in range(2):
            part = logits[:, side * FEAT : (side + 1) * FEAT]
            low_top = jnp.max(jnp.where(group, part, -jnp.inf), axis=-1, keepdims=True)
            high_top = jnp.max(jnp.where(group, -jnp.inf, part), axis=-1, keepdims=True)
            sides.append(jnp.exp(part - jnp.where(group, low_top, high_top)))
        raised = jnp.concatenate(sides, axis=-1)
        phi = (raised / mm(raised.astype(bfloat), ones)).astype(bfloat)
        phi_ref[:, h * 2 * FEAT : (h + 1) * 2 * FEAT] = phi
        extended = jnp.concatenate([value[:, h * HEAD : (h + 1) * HEAD], tail], axis=-1)
        vx_ref[:, h * FEAT : (h + 1) * FEAT] = extended
        tot_ref[h] = mm_tn(phi[:, FEAT:], extended).astype(bfloat)


def attend_kernel(
    x_ref, gain_ref, s_ref, phi_ref, vx_ref, state_ref, att_ref, inv_ref, middle_ref, normed_ref
):
    heads = state_ref.shape[0]
    tokens = x_ref.shape[0]
    keep = causal_keep(tokens)
    step = pl.program_id(0)

    @pl.when(step == 0)
    def _():
        middle_ref[...] = x_ref[...].astype(single)

    parts = []
    for h in range(heads):
        phi_q = phi_ref[:, h * 2 * FEAT : h * 2 * FEAT + FEAT]
        phi_k = phi_ref[:, h * 2 * FEAT + FEAT : (h + 1) * 2 * FEAT]
        scores = jnp.where(keep, mm_nt(phi_q, phi_k), 0.0).astype(bfloat)
        total = mm(scores, vx_ref[:, h * FEAT : (h + 1) * FEAT]) + mm(phi_q, state_ref[h])
        inverse = jnp.broadcast_to(1.0 / total[:, HEAD : HEAD + 1], (tokens, HEAD))
        inv_ref[0, :, h * HEAD : (h + 1) * HEAD] = inverse
        parts.append((total[:, :HEAD] * inverse).astype(bfloat))
    attended = jnp.concatenate(parts, axis=-1)
    att_ref[0] = attended
    base = heads * 3 * HEAD
    middle_ref[...] += mm_nt(attended, s_ref[:, base : base + heads * HEAD])

    @pl.when(step == pl.num_programs(0) - 1)
    def _():
        unit, _ = norm_parts(middle_ref[...])
        normed_ref[...] = (unit * gain_ref[...]).astype(bfloat)


def feed_kernel(
    middle_ref, gain_ref, normed_ref, cot_ref, u_ref, d_ref,
    out_ref, dmid_ref, branch_ref, gsum_ref, ug_ref, dg_ref, acc_ref,
):
    step = pl.program_id(0)
    normed = normed_ref[...]
    cot = cot_ref[...]
    upper = mm(normed, u_ref[...])
    square = upper * upper
    factor = 0.7978845608028654
    bent = jnp.tanh(factor * upper * (1.0 + 0.044715 * square))
    half = 0.5 * (1.0 + bent)
    hidden = (upper * half).astype(bfloat)
    slope = half + 0.5 * upper * (1.0 - bent * bent) * (
        factor * (1.0 + 3.0 * 0.044715 * square)
    )
    d_upper = (mm(cot, d_ref[...]) * slope).astype(bfloat)
    ug_ref[...] = mm_tn(normed, d_upper).astype(bfloat)
    dg_ref[...] = mm_tn(cot, hidden).astype(bfloat)
    more = mm_nt(hidden, d_ref[...])
    back = mm_nt(d_upper, u_ref[...])

    @pl.when(step == 0)
    def _():
        out_ref[...] = middle_ref[...] + more
        acc_ref[...] = back

    @pl.when(step > 0)
    def _():
        out_ref[...] += more
        acc_ref[...] += back

    @pl.when(step == pl.num_programs(0) - 1)
    def _():
        unit, scale = norm_parts(middle_ref[...])
        grad = acc_ref[...]
        gsum_ref[...] = jnp.sum(grad * unit, axis=0, keepdims=True)
        d_middle = cot.astype(single) + norm_back(unit, scale, grad, gain_ref[...])
        dmid_ref[...] = d_middle
        branch_ref[...] = d_middle.astype(bfloat)


def ratio_kernel(branch_ref, s_ref, att_ref, inv_ref, phi_ref, dn_ref, tot_ref):
    heads = tot_ref.shape[0]
    tokens = branch_ref.shape[0]
    base = heads * 3 * HEAD
    d_att = mm(branch_ref[...], s_ref[:, base : base + heads * HEAD])
    inverse = inv_ref[0]
    d_num = d_att * inverse
    against = d_num * att_ref[0].astype(single)
    lane = lax.broadcasted_iota(jnp.int32, (tokens, HEAD), 1)
    for h in range(heads):
        here = slice(h * HEAD, (h + 1) * HEAD)
        d_den = -jnp.sum(against[:, here], axis=-1, keepdims=True)
        high = d_den.astype(bfloat).astype(single)
        tail = jnp.where(lane == 0, high, jnp.where(lane == 1, d_den - high, 0.0))
        extended = jnp.concatenate([d_num[:, here], tail], axis=-1).astype(bfloat)
        dn_ref[:, h * FEAT : (h + 1) * FEAT] = extended
        tot_ref[h] = mm_tn(phi_ref[:, h * 2 * FEAT : h * 2 * FEAT + FEAT], extended).astype(bfloat)


def back_kernel(
    x_ref, gain_ref, normed_ref, dmid_ref, branch_ref, s_ref, f_ref, att_ref,
    qk_ref, phi_ref, vx_ref, dn_ref, state_ref, later_ref,
    tg_ref, gsum_ref, sg_ref, fg_ref, acc_ref,
):
    step = pl.program_id(0)
    heads = state_ref.shape[0]
    tokens = x_ref.shape[0]
    keep = causal_keep(tokens)
    ones = half_ones(2 * FEAT)
    pairs = []
    values = []
    for h in range(heads):
        phi_q = phi_ref[:, h * 2 * FEAT : h * 2 * FEAT + FEAT]
        phi_k = phi_ref[:, h * 2 * FEAT + FEAT : (h + 1) * 2 * FEAT]
        extended = vx_ref[:, h * FEAT : (h + 1) * FEAT]
        d_num = dn_ref[:, h * FEAT : (h + 1) * FEAT]
        scores = jnp.where(keep, mm_nt(phi_q, phi_k), 0.0).astype(bfloat)
        d_scores = jnp.where(keep, mm_nt(d_num, extended), 0.0).astype(bfloat)
        d_phi_q = mm(d_scores, phi_k) + mm_nt(d_num, state_ref[h])
        d_phi_k = mm_tn(d_scores, phi_q) + mm_nt(extended, later_ref[h])
        d_value = mm_tn(scores, d_num) + mm(phi_k, later_ref[h])
        values.append(d_value[:, :HEAD].astype(bfloat))
        d_phi = jnp.concatenate([d_phi_q, d_phi_k], axis=-1)
        phi = phi_ref[:, h * 2 * FEAT : (h + 1) * 2 * FEAT].astype(single)
        high, rest = split_low(d_phi * phi)
        mean = mm(high, ones) + mm(rest, ones)
        d_logits = (phi * (d_phi - mean)).astype(bfloat)
        pairs.append(mm_nt(d_logits, f_ref[h]).astype(bfloat))
        cross = mm_tn(qk_ref[:, h * FEAT : (h + 1) * FEAT], d_logits)
        fg_ref[h] = (
            cross[:HEAD, :HEAD]
            - cross[:HEAD, HEAD:FEAT]
            + cross[HEAD:, FEAT : FEAT + HEAD]
            - cross[HEAD:, FEAT + HEAD :]
        )
    projected = jnp.concatenate(pairs + values, axis=-1)
    width = heads * 3 * HEAD
    sg_ref[...] = jnp.concatenate(
        [mm_tn(normed_ref[...], projected), mm_tn(branch_ref[...], att_ref[0])], axis=-1
    ).astype(bfloat)
    more = mm_nt(projected, s_ref[:, :width])

    @pl.when(step == 0)
    def _():
        acc_ref[...] = more

    @pl.when(step > 0)
    def _():
        acc_ref[...] += more

    @pl.when(step == pl.num_programs(0) - 1)
    def _():
        unit, scale = norm_parts(x_ref[...].astype(single))
        grad = acc_ref[...]
        gsum_ref[...] = jnp.sum(grad * unit, axis=0, keepdims=True)
        tg_ref[...] = dmid_ref[...] + norm_back(unit, scale, grad, gain_ref[...])


def whole(array):
    return pl.BlockSpec(array.shape, lambda j: (0,) * len(array.shape))


def columns(array, groups):
    return pl.BlockSpec((array.shape[0], array.shape[1] // groups), lambda j: (0, j))


def leading(array, groups):
    rest = array.shape[1:]
    return pl.BlockSpec(
        (array.shape[0] // groups,) + rest, lambda j: (j,) + (0,) * len(rest)
    )


def stage(kernel, groups, inputs, outputs, scratch=()):
    kinds = {"w": lambda a, g: whole(a), "c": columns, "l": leading}
    return pl.pallas_call(
        kernel,
        grid=(groups,),
        in_specs=[kinds[kind](array, groups) for kind, array in inputs],
        out_specs=[
            kinds[kind](jax.ShapeDtypeStruct(shape, dtype), groups)
            for kind, shape, dtype in outputs
        ],
        out_shape=[jax.ShapeDtypeStruct(shape, dtype) for kind, shape, dtype in outputs],
        scratch_shapes=list(scratch),
        compiler_params=pltpu.CompilerParams(
            dimension_semantics=("arbitrary",), vmem_limit_bytes=LIMIT
        ),
    )(*[array for kind, array in inputs])


def state_before(totals, groups, later):
    every = lax.all_gather(totals, "tensor", axis=0)
    me = lax.axis_index("tensor")
    order = jnp.arange(groups)
    chosen = (order > me) if later else (order < me)
    shape = (groups,) + (1,) * totals.ndim
    return jnp.sum(
        jnp.where(chosen.reshape(shape), every.astype(single), 0.0), axis=0
    ).astype(bfloat)


def compute(groups, tokens, cotangent, gain_one, gain_two, feature, square, up, down):
    length, width = tokens.shape
    heads = feature.shape[0]
    zero = jnp.zeros_like(feature)
    top = jnp.concatenate([feature, -feature, zero, zero], axis=2)
    low = jnp.concatenate([zero, zero, feature, -feature], axis=2)
    maps = jnp.concatenate([top, low], axis=1)
    feat_all = heads * 2 * FEAT
    ext_all = heads * FEAT
    head_block = (groups, length, heads // groups * HEAD)
    normed, pair, phi, extended, totals = stage(
        features_kernel, groups,
        [("w", tokens), ("w", gain_one), ("c", square), ("l", maps)],
        [("w", (length, width), bfloat), ("c", (length, ext_all), bfloat),
         ("c", (length, feat_all), bfloat), ("c", (length, ext_all), bfloat),
         ("l", (heads, FEAT, FEAT), bfloat)],
    )
    before = state_before(totals, groups, False)
    attended, inverse, middle, normed_two = stage(
        attend_kernel, groups,
        [("w", tokens), ("w", gain_two), ("c", square), ("c", phi), ("c", extended), ("l", before)],
        [("l", head_block, bfloat), ("l", head_block, single),
         ("w", (length, width), single), ("w", (length, width), bfloat)],
    )
    block_out, d_middle, branch, gain_two_sum, up_grad, down_grad = stage(
        feed_kernel, groups,
        [("w", middle), ("w", gain_two), ("w", normed_two), ("w", cotangent), ("c", up), ("c", down)],
        [("w", (length, width), single), ("w", (length, width), single),
         ("w", (length, width), bfloat), ("w", (1, width), single),
         ("c", up.shape, bfloat), ("c", down.shape, bfloat)],
        [pltpu.VMEM((length, width), single)],
    )
    d_num, d_totals = stage(
        ratio_kernel, groups,
        [("w", branch), ("c", square), ("l", attended), ("l", inverse), ("c", phi)],
        [("c", (length, ext_all), bfloat), ("l", (heads, FEAT, FEAT), bfloat)],
    )
    after = state_before(d_totals, groups, True)
    tokens_grad, gain_one_sum, square_grad, feature_grad = stage(
        back_kernel, groups,
        [("w", tokens), ("w", gain_one), ("w", normed), ("w", d_middle), ("w", branch),
         ("c", square), ("l", maps), ("l", attended), ("c", pair), ("c", phi), ("c", extended),
         ("c", d_num), ("l", before), ("l", after)],
        [("w", (length, width), single), ("w", (1, width), single),
         ("c", square.shape, bfloat), ("l", feature.shape, single)],
        [pltpu.VMEM((length, width), single)],
    )
    return (
        block_out, tokens_grad, gain_one_sum, gain_two_sum,
        square_grad, feature_grad, up_grad, down_grad,
    )


def pack_square(qkv, out_weight):
    rows = qkv.shape[1]
    heads = qkv.shape[2] // HEAD
    query = qkv[0].reshape(rows, heads, 1, HEAD)
    key = qkv[1].reshape(rows, heads, 1, HEAD)
    pair = jnp.concatenate([query, key], axis=2).reshape(rows, heads * 2 * HEAD)
    return jnp.concatenate([pair, qkv[2], out_weight.T], axis=1)


def unpack_square(grad):
    rows, width = grad.shape
    part = width // 4
    heads = part // HEAD
    pair = grad[:, : 2 * part].reshape(rows, heads, 2, HEAD)
    query = pair[:, :, 0].reshape(rows, part)
    key = pair[:, :, 1].reshape(rows, part)
    return jnp.stack([query, key, grad[:, 2 * part : 3 * part]]), grad[:, 3 * part :].T


def per_device(
    groups, dp, tokens, gain_one, gain_two, qkv_weight, feature_weight, out_weight, up_weight,
    down_weight, cotangent,
):
    def gathered(block):
        rows = lax.all_gather(block, "dp", axis=0, tiled=True)
        return lax.all_gather(rows, "tensor", axis=1, tiled=True)

    def scattered(grad):
        rows = lax.psum_scatter(grad, "tensor", scatter_dimension=1, tiled=True)
        return lax.psum_scatter(rows, "dp", scatter_dimension=0, tiled=True).astype(single)

    square = gathered(pack_square(qkv_weight.astype(bfloat), out_weight.astype(bfloat)))
    up = gathered(up_weight.astype(bfloat))
    down = gathered(down_weight.astype(bfloat).T)
    feature = lax.all_gather(feature_weight.astype(bfloat), "dp", axis=1, tiled=True)
    feature = lax.all_gather(feature, "tensor", axis=0, tiled=True)
    gain_first = lax.all_gather(gain_one.astype(bfloat), "dp", axis=0, tiled=True)
    gain_second = lax.all_gather(gain_two.astype(bfloat), "dp", axis=0, tiled=True)
    (
        block_out, tokens_grad, gain_one_sum, gain_two_sum,
        square_grad, feature_grad, up_grad, down_grad,
    ) = compute(
        groups, tokens, cotangent, gain_first.astype(single)[None], gain_second.astype(single)[None],
        feature, square, up, down,
    )
    qkv_grad, out_grad = unpack_square(scattered(square_grad))
    up_out = scattered(up_grad)
    down_out = scattered(down_grad).T
    feature_out = lax.psum_scatter(feature_grad, "tensor", scatter_dimension=0, tiled=True)
    feature_out = lax.psum_scatter(feature_out, "dp", scatter_dimension=1, tiled=True)
    gains = lax.psum(jnp.concatenate([gain_one_sum[0], gain_two_sum[0]]), ("tensor", "dp"))
    rows = gain_one.shape[0]
    place = lax.axis_index("dp") * rows
    gain_one_out = lax.dynamic_slice(gains, (place,), (rows,))
    gain_two_out = lax.dynamic_slice(gains, (place + rows * dp,), (rows,))
    return (
        block_out, tokens_grad, gain_one_out, gain_two_out, qkv_grad, feature_out, out_grad,
        up_out, down_out,
    )


def solution(mesh):
    return jax.shard_map(
        functools.partial(per_device, mesh.shape["tensor"], mesh.shape["dp"]),
        mesh=mesh,
        in_specs=(
            P(("dp", "tensor"), None),
            P("dp"),
            P("dp"),
            P(None, "dp", "tensor"),
            P("tensor", "dp", None),
            P("tensor", "dp"),
            P("dp", "tensor"),
            P("tensor", "dp"),
            P(("dp", "tensor"), None),
        ),
        out_specs=(
            P(("dp", "tensor"), None),
            P(("dp", "tensor"), None),
            P("dp"),
            P("dp"),
            P(None, "dp", "tensor"),
            P("tensor", "dp", None),
            P("tensor", "dp"),
            P("dp", "tensor"),
            P("tensor", "dp"),
        ),
        check_vma=False,
    )
```

```python
import functools

import jax
import jax.numpy as jnp
from jax import lax
from jax.experimental import pallas as pl
from jax.experimental.pallas import tpu as pltpu
from jax.sharding import PartitionSpec as P

bfloat = jnp.bfloat16
single = jnp.float32
EPSILON = 1e-5
HEAD = 64
FEAT = 128
LIMIT = 64000000


def mm(left, right):
    return jnp.dot(left, right, preferred_element_type=single)


def mm_tn(left, right):
    return lax.dot_general(left, right, (((0,), (0,)), ((), ())), preferred_element_type=single)


def mm_nt(left, right):
    return lax.dot_general(left, right, (((1,), (1,)), ((), ())), preferred_element_type=single)


def norm_parts(rows):
    center = rows - jnp.mean(rows, axis=-1, keepdims=True)
    spread = jnp.mean(center * center, axis=-1, keepdims=True)
    scale = lax.rsqrt(spread + EPSILON)
    return center * scale, scale


def norm_back(unit, scale, grad, gain):
    scaled = grad * gain
    return scale * (
        scaled
        - jnp.mean(scaled, axis=-1, keepdims=True)
        - unit * jnp.mean(scaled * unit, axis=-1, keepdims=True)
    )


def split_low(values):
    high = values.astype(bfloat)
    return high, (values - high.astype(single)).astype(bfloat)


def half_ones(width):
    row = lax.broadcasted_iota(jnp.int32, (width, width), 0) // HEAD
    column = lax.broadcasted_iota(jnp.int32, (width, width), 1) // HEAD
    return (row == column).astype(single).astype(bfloat)


def causal_keep(length):
    row = lax.broadcasted_iota(jnp.int32, (length, length), 0)
    column = lax.broadcasted_iota(jnp.int32, (length, length), 1)
    return column <= row


def features_kernel(x_ref, gain_ref, s_ref, f_ref, normed_ref, qk_ref, phi_ref, vx_ref, tot_ref):
    @pl.when(pl.program_id(0) == 0)
    def _():
        unit, _ = norm_parts(x_ref[...].astype(single))
        normed_ref[...] = (unit * gain_ref[...]).astype(bfloat)

    normed = normed_ref[...]
    heads = f_ref.shape[0]
    tokens = normed.shape[0]
    qk_width = heads * 2 * HEAD
    ones = half_ones(2 * FEAT)
    lane = lax.broadcasted_iota(jnp.int32, (1, HEAD), 1)
    tail = jnp.broadcast_to((lane < 2).astype(single).astype(bfloat), (tokens, HEAD))
    group = lax.broadcasted_iota(jnp.int32, (1, FEAT), 1) < HEAD
    value = mm(normed, s_ref[:, qk_width : qk_width + heads * HEAD]).astype(bfloat)
    for h in range(heads):
        pair = mm(normed, s_ref[:, h * FEAT : (h + 1) * FEAT])
        high, rest = split_low(pair)
        qk_ref[:, h * FEAT : (h + 1) * FEAT] = high
        logits = mm(high, f_ref[h]) + mm(rest, f_ref[h])
        sides = []
        for side in range(2):
            part = logits[:, side * FEAT : (side + 1) * FEAT]
            low_top = jnp.max(jnp.where(group, part, -jnp.inf), axis=-1, keepdims=True)
            high_top = jnp.max(jnp.where(group, -jnp.inf, part), axis=-1, keepdims=True)
            sides.append(jnp.exp(part - jnp.where(group, low_top, high_top)))
        raised = jnp.concatenate(sides, axis=-1)
        phi = (raised / mm(raised.astype(bfloat), ones)).astype(bfloat)
        phi_ref[:, h * 2 * FEAT : (h + 1) * 2 * FEAT] = phi
        extended = jnp.concatenate([value[:, h * HEAD : (h + 1) * HEAD], tail], axis=-1)
        vx_ref[:, h * FEAT : (h + 1) * FEAT] = extended
        tot_ref[h] = mm_tn(phi[:, FEAT:], extended).astype(bfloat)


def attend_kernel(
    x_ref, gain_ref, s_ref, phi_ref, vx_ref, state_ref, att_ref, inv_ref, middle_ref, normed_ref
):
    heads = state_ref.shape[0]
    tokens = x_ref.shape[0]
    keep = causal_keep(tokens)
    step = pl.program_id(0)

    @pl.when(step == 0)
    def _():
        middle_ref[...] = x_ref[...].astype(single)

    parts = []
    for h in range(heads):
        phi_q = phi_ref[:, h * 2 * FEAT : h * 2 * FEAT + FEAT]
        phi_k = phi_ref[:, h * 2 * FEAT + FEAT : (h + 1) * 2 * FEAT]
        scores = jnp.where(keep, mm_nt(phi_q, phi_k), 0.0).astype(bfloat)
        total = mm(scores, vx_ref[:, h * FEAT : (h + 1) * FEAT]) + mm(phi_q, state_ref[h])
        inverse = jnp.broadcast_to(1.0 / total[:, HEAD : HEAD + 1], (tokens, HEAD))
        inv_ref[0, :, h * HEAD : (h + 1) * HEAD] = inverse
        parts.append((total[:, :HEAD] * inverse).astype(bfloat))
    attended = jnp.concatenate(parts, axis=-1)
    att_ref[0] = attended
    base = heads * 3 * HEAD
    middle_ref[...] += mm_nt(attended, s_ref[:, base : base + heads * HEAD])

    @pl.when(step == pl.num_programs(0) - 1)
    def _():
        unit, _ = norm_parts(middle_ref[...])
        normed_ref[...] = (unit * gain_ref[...]).astype(bfloat)


def feed_kernel(
    middle_ref, gain_ref, normed_ref, cot_ref, u_ref, d_ref,
    out_ref, dmid_ref, branch_ref, gsum_ref, ug_ref, dg_ref, acc_ref,
):
    step = pl.program_id(0)
    normed = normed_ref[...]
    cot = cot_ref[...]
    upper = mm(normed, u_ref[...])
    square = upper * upper
    factor = 0.7978845608028654
    bent = jnp.tanh(factor * upper * (1.0 + 0.044715 * square))
    half = 0.5 * (1.0 + bent)
    hidden = (upper * half).astype(bfloat)
    slope = half + 0.5 * upper * (1.0 - bent * bent) * (
        factor * (1.0 + 3.0 * 0.044715 * square)
    )
    d_upper = (mm(cot, d_ref[...]) * slope).astype(bfloat)
    ug_ref[...] = mm_tn(normed, d_upper).astype(bfloat)
    dg_ref[...] = mm_tn(cot, hidden).astype(bfloat)
    more = mm_nt(hidden, d_ref[...])
    back = mm_nt(d_upper, u_ref[...])

    @pl.when(step == 0)
    def _():
        out_ref[...] = middle_ref[...] + more
        acc_ref[...] = back

    @pl.when(step > 0)
    def _():
        out_ref[...] += more
        acc_ref[...] += back

    @pl.when(step == pl.num_programs(0) - 1)
    def _():
        unit, scale = norm_parts(middle_ref[...])
        grad = acc_ref[...]
        gsum_ref[...] = jnp.sum(grad * unit, axis=0, keepdims=True)
        d_middle = cot.astype(single) + norm_back(unit, scale, grad, gain_ref[...])
        dmid_ref[...] = d_middle
        branch_ref[...] = d_middle.astype(bfloat)


def ratio_kernel(branch_ref, s_ref, att_ref, inv_ref, phi_ref, dn_ref, tot_ref):
    heads = tot_ref.shape[0]
    tokens = branch_ref.shape[0]
    base = heads * 3 * HEAD
    d_att = mm(branch_ref[...], s_ref[:, base : base + heads * HEAD])
    inverse = inv_ref[0]
    d_num = d_att * inverse
    against = d_num * att_ref[0].astype(single)
    lane = lax.broadcasted_iota(jnp.int32, (tokens, HEAD), 1)
    for h in range(heads):
        here = slice(h * HEAD, (h + 1) * HEAD)
        d_den = -jnp.sum(against[:, here], axis=-1, keepdims=True)
        high = d_den.astype(bfloat).astype(single)
        tail = jnp.where(lane == 0, high, jnp.where(lane == 1, d_den - high, 0.0))
        extended = jnp.concatenate([d_num[:, here], tail], axis=-1).astype(bfloat)
        dn_ref[:, h * FEAT : (h + 1) * FEAT] = extended
        tot_ref[h] = mm_tn(phi_ref[:, h * 2 * FEAT : h * 2 * FEAT + FEAT], extended).astype(bfloat)


def back_kernel(
    x_ref, gain_ref, normed_ref, dmid_ref, branch_ref, s_ref, f_ref, att_ref,
    qk_ref, phi_ref, vx_ref, dn_ref, state_ref, later_ref,
    tg_ref, gsum_ref, sg_ref, fg_ref, acc_ref,
):
    step = pl.program_id(0)
    heads = state_ref.shape[0]
    tokens = x_ref.shape[0]
    keep = causal_keep(tokens)
    ones = half_ones(2 * FEAT)
    pairs = []
    values = []
    for h in range(heads):
        phi_q = phi_ref[:, h * 2 * FEAT : h * 2 * FEAT + FEAT]
        phi_k = phi_ref[:, h * 2 * FEAT + FEAT : (h + 1) * 2 * FEAT]
        extended = vx_ref[:, h * FEAT : (h + 1) * FEAT]
        d_num = dn_ref[:, h * FEAT : (h + 1) * FEAT]
        scores = jnp.where(keep, mm_nt(phi_q, phi_k), 0.0).astype(bfloat)
        d_scores = jnp.where(keep, mm_nt(d_num, extended), 0.0).astype(bfloat)
        d_phi_q = mm(d_scores, phi_k) + mm_nt(d_num, state_ref[h])
        d_phi_k = mm_tn(d_scores, phi_q) + mm_nt(extended, later_ref[h])
        d_value = mm_tn(scores, d_num) + mm(phi_k, later_ref[h])
        values.append(d_value[:, :HEAD].astype(bfloat))
        d_phi = jnp.concatenate([d_phi_q, d_phi_k], axis=-1)
        phi = phi_ref[:, h * 2 * FEAT : (h + 1) * 2 * FEAT].astype(single)
        high, rest = split_low(d_phi * phi)
        mean = mm(high, ones) + mm(rest, ones)
        d_logits = (phi * (d_phi - mean)).astype(bfloat)
        pairs.append(mm_nt(d_logits, f_ref[h]).astype(bfloat))
        cross = mm_tn(qk_ref[:, h * FEAT : (h + 1) * FEAT], d_logits)
        fg_ref[h] = (
            cross[:HEAD, :HEAD]
            - cross[:HEAD, HEAD:FEAT]
            + cross[HEAD:, FEAT : FEAT + HEAD]
            - cross[HEAD:, FEAT + HEAD :]
        )
    projected = jnp.concatenate(pairs + values, axis=-1)
    width = heads * 3 * HEAD
    sg_ref[...] = jnp.concatenate(
        [mm_tn(normed_ref[...], projected), mm_tn(branch_ref[...], att_ref[0])], axis=-1
    ).astype(bfloat)
    more = mm_nt(projected, s_ref[:, :width])

    @pl.when(step == 0)
    def _():
        acc_ref[...] = more

    @pl.when(step > 0)
    def _():
        acc_ref[...] += more

    @pl.when(step == pl.num_programs(0) - 1)
    def _():
        unit, scale = norm_parts(x_ref[...].astype(single))
        grad = acc_ref[...]
        gsum_ref[...] = jnp.sum(grad * unit, axis=0, keepdims=True)
        tg_ref[...] = dmid_ref[...] + norm_back(unit, scale, grad, gain_ref[...])


def whole(array):
    return pl.BlockSpec(array.shape, lambda j: (0,) * len(array.shape))


def columns(array, groups):
    return pl.BlockSpec((array.shape[0], array.shape[1] // groups), lambda j: (0, j))


def leading(array, groups):
    rest = array.shape[1:]
    return pl.BlockSpec(
        (array.shape[0] // groups,) + rest, lambda j: (j,) + (0,) * len(rest)
    )


def stage(kernel, groups, inputs, outputs, scratch=()):
    kinds = {"w": lambda a, g: whole(a), "c": columns, "l": leading}
    return pl.pallas_call(
        kernel,
        grid=(groups,),
        in_specs=[kinds[kind](array, groups) for kind, array in inputs],
        out_specs=[
            kinds[kind](jax.ShapeDtypeStruct(shape, dtype), groups)
            for kind, shape, dtype in outputs
        ],
        out_shape=[jax.ShapeDtypeStruct(shape, dtype) for kind, shape, dtype in outputs],
        scratch_shapes=list(scratch),
        compiler_params=pltpu.CompilerParams(
            dimension_semantics=("arbitrary",), vmem_limit_bytes=LIMIT
        ),
    )(*[array for kind, array in inputs])


def state_before(totals, groups, later):
    every = lax.all_gather(totals, "tensor", axis=0)
    me = lax.axis_index("tensor")
    order = jnp.arange(groups)
    chosen = (order > me) if later else (order < me)
    shape = (groups,) + (1,) * totals.ndim
    return jnp.sum(
        jnp.where(chosen.reshape(shape), every.astype(single), 0.0), axis=0
    ).astype(bfloat)


def compute(groups, tokens, cotangent, gain_one, gain_two, feature, square, up, down):
    length, width = tokens.shape
    heads = feature.shape[0]
    zero = jnp.zeros_like(feature)
    top = jnp.concatenate([feature, -feature, zero, zero], axis=2)
    low = jnp.concatenate([zero, zero, feature, -feature], axis=2)
    maps = jnp.concatenate([top, low], axis=1)
    feat_all = heads * 2 * FEAT
    ext_all = heads * FEAT
    head_block = (groups, length, heads // groups * HEAD)
    normed, pair, phi, extended, totals = stage(
        features_kernel, groups,
        [("w", tokens), ("w", gain_one), ("c", square), ("l", maps)],
        [("w", (length, width), bfloat), ("c", (length, ext_all), bfloat),
         ("c", (length, feat_all), bfloat), ("c", (length, ext_all), bfloat),
         ("l", (heads, FEAT, FEAT), bfloat)],
    )
    before = state_before(totals, groups, False)
    attended, inverse, middle, normed_two = stage(
        attend_kernel, groups,
        [("w", tokens), ("w", gain_two), ("c", square), ("c", phi), ("c", extended), ("l", before)],
        [("l", head_block, bfloat), ("l", head_block, single),
         ("w", (length, width), single), ("w", (length, width), bfloat)],
    )
    block_out, d_middle, branch, gain_two_sum, up_grad, down_grad = stage(
        feed_kernel, groups,
        [("w", middle), ("w", gain_two), ("w", normed_two), ("w", cotangent), ("c", up), ("c", down)],
        [("w", (length, width), single), ("w", (length, width), single),
         ("w", (length, width), bfloat), ("w", (1, width), single),
         ("c", up.shape, bfloat), ("c", down.shape, bfloat)],
        [pltpu.VMEM((length, width), single)],
    )
    d_num, d_totals = stage(
        ratio_kernel, groups,
        [("w", branch), ("c", square), ("l", attended), ("l", inverse), ("c", phi)],
        [("c", (length, ext_all), bfloat), ("l", (heads, FEAT, FEAT), bfloat)],
    )
    after = state_before(d_totals, groups, True)
    tokens_grad, gain_one_sum, square_grad, feature_grad = stage(
        back_kernel, groups,
        [("w", tokens), ("w", gain_one), ("w", normed), ("w", d_middle), ("w", branch),
         ("c", square), ("l", maps), ("l", attended), ("c", pair), ("c", phi), ("c", extended),
         ("c", d_num), ("l", before), ("l", after)],
        [("w", (length, width), single), ("w", (1, width), single),
         ("c", square.shape, bfloat), ("l", feature.shape, single)],
        [pltpu.VMEM((length, width), single)],
    )
    return (
        block_out, tokens_grad, gain_one_sum, gain_two_sum,
        square_grad, feature_grad, up_grad, down_grad,
    )


def pack_square(qkv, out_weight):
    rows = qkv.shape[1]
    heads = qkv.shape[2] // HEAD
    query = qkv[0].reshape(rows, heads, 1, HEAD)
    key = qkv[1].reshape(rows, heads, 1, HEAD)
    pair = jnp.concatenate([query, key], axis=2).reshape(rows, heads * 2 * HEAD)
    return jnp.concatenate([pair, qkv[2], out_weight.T], axis=1)


def unpack_square(grad):
    rows, width = grad.shape
    part = width // 4
    heads = part // HEAD
    pair = grad[:, : 2 * part].reshape(rows, heads, 2, HEAD)
    query = pair[:, :, 0].reshape(rows, part)
    key = pair[:, :, 1].reshape(rows, part)
    return jnp.stack([query, key, grad[:, 2 * part : 3 * part]]), grad[:, 3 * part :].T


MESH = pl.DeviceIdType.MESH
LINE = 4


class Place:
    def __init__(self):
        share, spot = lax.axis_index("dp"), lax.axis_index("tensor")
        self.z, self.x = share // 2, lax.rem(share, 2)
        self.y, self.core = spot // 2, lax.rem(spot, 2)
        core = self.core
        near = (lax.rem(self.x + 1 - core, 2), lax.rem(self.y + core, 2))
        far = (lax.rem(self.x + core, 2), lax.rem(self.y + 1 - core, 2))
        self.sides = [(self.x, self.y), near, far, (1 - self.x, 1 - self.y)]

    def device(self, z, side, core):
        x, y = self.sides[side]
        return (z * 2 + x, y * 2 + core)

    def right(self):
        return self.device(self.z + 1, 0, self.core)

    def left(self):
        return self.device(self.z - 1, 0, self.core)

    def near(self):
        return self.device(self.z, 1, self.core)

    def far(self):
        return self.device(self.z, 2, self.core)

    def twin(self):
        return self.device(self.z, 0, 1 - self.core)

    def meet(self):
        barrier = pltpu.get_barrier_semaphore()

        def greet(who):
            pl.semaphore_signal(barrier, inc=1, device_id=who, device_id_type=MESH)

        greet(self.near())
        greet(self.far())
        greet(self.twin())

        @pl.when(self.z > 0)
        def _():
            greet(self.left())

        @pl.when(self.z < LINE - 1)
        def _():
            greet(self.right())

        ends = (self.z == 0) | (self.z == LINE - 1)

        @pl.when(ends)
        def _():
            pl.semaphore_wait(barrier, 4)

        @pl.when(jnp.logical_not(ends))
        def _():
            pl.semaphore_wait(barrier, 5)


def gather_kernel(count, *refs):
    blocks, full = refs[:count], refs[count : 2 * count]
    send_sem, recv_sem, local_sem = refs[2 * count :]
    place = Place()
    width = blocks[0].shape[1]
    used = [0] * count
    pending = []

    def slot(a, z, side, core):
        share, spot = place.device(z, side, core)
        return full[a].at[share, :, pl.ds(pl.multiple_of(spot * width, width), width)]

    def arrival(a, z, side, core):
        share, spot = place.device(z, side, core)
        return recv_sem.at[a, share * 4 + spot]

    def send(a, source, z, side, who, valid):
        index = used[a]
        used[a] += 1
        copy = pltpu.make_async_remote_copy(
            src_ref=source,
            dst_ref=slot(a, z, side, place.core),
            send_sem=send_sem.at[a, index],
            recv_sem=arrival(a, z, side, place.core),
            device_id=who,
            device_id_type=MESH,
        )
        when(valid, copy.start)
        pending.append((valid, copy))

    def when(valid, action):
        if valid is None:
            action()
        else:
            pl.when(valid)(action)

    def wait(a, z, side, core, valid):
        here = slot(a, z, side, core)
        copy = pltpu.make_async_remote_copy(
            src_ref=here,
            dst_ref=here,
            send_sem=send_sem.at[a, 0],
            recv_sem=arrival(a, z, side, core),
            device_id=place.twin(),
            device_id_type=MESH,
        )
        when(valid, copy.wait_recv)

    place.meet()
    local = []
    for a in range(count):
        keep = pltpu.make_async_copy(
            blocks[a], slot(a, place.z, 0, place.core), local_sem.at[a]
        )
        keep.start()
        local.append(keep)
        send(a, blocks[a], place.z, 0, place.right(), place.z < LINE - 1)
        send(a, blocks[a], place.z, 0, place.left(), place.z > 0)
        send(a, blocks[a], place.z, 0, place.near(), None)
        send(a, blocks[a], place.z, 0, place.far(), None)
        send(a, blocks[a], place.z, 0, place.twin(), None)

    def line_task(a, offset):
        z = place.z + offset
        valid = (z >= 0) & (z < LINE)
        wait(a, z, 0, place.core, valid)
        here = slot(a, z, 0, place.core)
        if offset < 0:
            send(a, here, z, 0, place.right(), valid & (place.z < LINE - 1))
        else:
            send(a, here, z, 0, place.left(), valid & (place.z > 0))
        send(a, here, z, 0, place.near(), valid)
        send(a, here, z, 0, place.far(), valid)
        send(a, here, z, 0, place.twin(), valid)

    def side_task(a, offset, side):
        z = place.z + offset
        valid = None if offset == 0 else (z >= 0) & (z < LINE)
        wait(a, z, side, place.core, valid)
        here = slot(a, z, side, place.core)
        if side == 1:
            send(a, here, z, side, place.far(), valid)
        send(a, here, z, side, place.twin(), valid)

    for hop in range(1, LINE + 2):
        for a in range(count):
            for side, delay in ((0, 0), (1, 1), (2, 1), (3, 2)):
                reach = hop - delay
                if reach < 0 or reach >= LINE or (side == 0 and reach == 0):
                    continue
                for offset in (0,) if reach == 0 else (-reach, reach):
                    if side == 0:
                        line_task(a, offset)
                    else:
                        side_task(a, offset, side)
    for a in range(count):
        for z in range(LINE):
            for side in range(4):
                wait(a, z, side, 1 - place.core, None)
    for keep in local:
        keep.wait()
    for valid, copy in pending:
        when(valid, copy.wait_send)


def scatter_kernel(count, *refs):
    grads, sums = refs[:count], refs[count : 2 * count]
    rest = refs[2 * count :]
    buffers = [rest[6 * a : 6 * a + 6] for a in range(count)]
    send_sem, recv_sem, local_sem = rest[6 * count :]
    place = Place()
    width = sums[0].shape[1]
    used = [0] * count
    pending = []

    def when(valid, action):
        if valid is None:
            action()
        else:
            pl.when(valid)(action)

    def part(a, z, side, core):
        share, spot = place.device(z, side, core)
        return grads[a].at[share, :, pl.ds(pl.multiple_of(spot * width, width), width)]

    def send(a, source, target, arrival, who, valid=None):
        index = used[a]
        used[a] += 1
        copy = pltpu.make_async_remote_copy(
            src_ref=source,
            dst_ref=target,
            send_sem=send_sem.at[a, index],
            recv_sem=recv_sem.at[a, arrival],
            device_id=who,
            device_id_type=MESH,
        )
        when(valid, copy.start)
        pending.append((valid, copy))

    def wait(a, target, arrival, valid=None):
        copy = pltpu.make_async_remote_copy(
            src_ref=target,
            dst_ref=target,
            send_sem=send_sem.at[a, 0],
            recv_sem=recv_sem.at[a, arrival],
            device_id=place.twin(),
            device_id_type=MESH,
        )
        when(valid, copy.wait_recv)

    place.meet()
    loads = {}
    swap = (0, 2, 1, 3)
    for a in range(count):
        mine, twin = buffers[a][0], buffers[a][1]
        for side in (3, 2, 1, 0):
            for z in range(LINE):
                index = side * LINE + z
                send(
                    a, part(a, z, swap[side], 1 - place.core), twin.at[index], index, place.twin()
                )
                load = pltpu.make_async_copy(
                    part(a, z, side, place.core), mine.at[index], local_sem.at[a, index]
                )
                load.start()
                loads[a, index] = load

    def join(a, index):
        mine, twin = buffers[a][0], buffers[a][1]
        loads[a, index].wait()
        wait(a, twin.at[index], index)
        return mine[index].astype(single) + twin[index].astype(single)

    def far_task(a):
        mine, far = buffers[a][0], buffers[a][2]
        for side, row in ((3, 1), (2, 0)):
            for z in range(LINE):
                index = side * LINE + z
                mine[index] = join(a, index).astype(bfloat)
                there = row * LINE + z
                send(a, mine.at[index], far.at[there], 16 + there, place.far())

    def near_task(a):
        mine, far, near = buffers[a][0], buffers[a][2], buffers[a][3]
        for z in range(LINE):
            index = LINE + z
            total = join(a, index)
            wait(a, far.at[LINE + z], 16 + LINE + z)
            mine[index] = (total + far[LINE + z].astype(single)).astype(bfloat)
            send(a, mine.at[index], near.at[z], 24 + z, place.near())

    def line_task(a):
        mine, _, far, near, left, right = buffers[a]
        for z in range(LINE):
            total = join(a, z)
            wait(a, far.at[z], 16 + z)
            total = total + far[z].astype(single)
            wait(a, near.at[z], 24 + z)
            mine[z] = (total + near[z].astype(single)).astype(bfloat)

            def onward(z, came, base, has, valid, who):
                @pl.when(valid & has)
                def _():
                    wait(a, came.at[z], base + z)
                    mine[z] = (mine[z].astype(single) + came[z].astype(single)).astype(bfloat)

                send(a, mine.at[z], came.at[z], base + z, who, valid)

            if z > 0:
                onward(z, left, 28, place.z > 0, place.z < z, place.right())
            if z < LINE - 1:
                onward(z, right, 32, place.z < LINE - 1, place.z > z, place.left())

    def last_task(a):
        mine, _, _, _, left, right = buffers[a]
        for z in range(LINE):

            @pl.when(place.z == z)
            def _(z=z):
                total = mine[z].astype(single)
                if z > 0:
                    wait(a, left.at[z], 28 + z)
                    total = total + left[z].astype(single)
                if z < LINE - 1:
                    wait(a, right.at[z], 32 + z)
                    total = total + right[z].astype(single)
                sums[a][...] = total

    tasks = (far_task, near_task, line_task, last_task)
    for wave in range(count + len(tasks) - 1):
        for level in reversed(range(len(tasks))):
            if 0 <= wave - level < count:
                tasks[level](wave - level)
    for valid, copy in pending:
        when(valid, copy.wait_send)


def gather_call(blocks, dp, groups):
    count = len(blocks)
    anywhere = pl.BlockSpec(memory_space=pl.ANY)
    return pl.pallas_call(
        functools.partial(gather_kernel, count),
        out_shape=[
            jax.ShapeDtypeStruct((dp, b.shape[0], groups * b.shape[1]), b.dtype) for b in blocks
        ],
        in_specs=[anywhere] * count,
        out_specs=[anywhere] * count,
        scratch_shapes=[
            pltpu.SemaphoreType.DMA((count, 64)),
            pltpu.SemaphoreType.DMA((count, dp * groups)),
            pltpu.SemaphoreType.DMA((count,)),
        ],
        compiler_params=pltpu.CompilerParams(collective_id=0, has_side_effects=True),
    )(*blocks)


def scatter_call(grads, dp, groups):
    count = len(grads)
    width = grads[0].shape[2] // groups
    slots = (16, 16, 8, 4, 4, 4)
    return pl.pallas_call(
        functools.partial(scatter_kernel, count),
        out_shape=[jax.ShapeDtypeStruct((g.shape[1], width), single) for g in grads],
        in_specs=[pl.BlockSpec(memory_space=pl.ANY)] * count,
        out_specs=[pl.BlockSpec(memory_space=pltpu.VMEM)] * count,
        scratch_shapes=[
            pltpu.VMEM((slot, g.shape[1], width), bfloat) for g in grads for slot in slots
        ]
        + [
            pltpu.SemaphoreType.DMA((count, 48)),
            pltpu.SemaphoreType.DMA((count, 36)),
            pltpu.SemaphoreType.DMA((count, 16)),
        ],
        compiler_params=pltpu.CompilerParams(
            collective_id=1, has_side_effects=True, vmem_limit_bytes=LIMIT
        ),
    )(*grads)


def kernel_gather(dp, groups, gain_one, gain_two, feature, square, up, down):
    width = square.shape[1]
    rows = gain_one.shape[0]
    small = jnp.concatenate(
        [feature.reshape(-1), gain_one, gain_two, jnp.zeros((width - 2 * rows,), bfloat)]
    ).reshape(-1, width)
    small = jnp.pad(small, ((0, 16 - small.shape[0]), (0, 0)))
    square, up, down, small = gather_call([square, up, down, small], dp, groups)
    full = [part.reshape(-1, groups * width) for part in (square, up, down)]
    heads, piece, size = feature.shape
    maps = small[:, :2].reshape(dp, 2, groups, width).transpose(2, 0, 1, 3)
    maps = maps.reshape(groups, dp, heads, piece, size).transpose(0, 2, 1, 3, 4)
    gains = small[:, 2, : 2 * rows]
    return (
        gains[:, :rows].reshape(1, -1),
        gains[:, rows:].reshape(1, -1),
        maps.reshape(groups * heads, dp * piece, size),
        *full,
    )


def kernel_scatter(dp, groups, gain_one, gain_two, feature, square, up, down):
    width = square.shape[1] // groups
    heads, _, size = feature.shape
    local = heads // groups
    piece = feature.shape[1] // dp
    maps = feature.reshape(groups, local, dp, piece, size).transpose(2, 0, 1, 3, 4)
    maps = maps.reshape(dp, groups, 2, width).transpose(0, 2, 1, 3).reshape(dp, 2, -1)
    rows = gain_one.shape[1] // dp
    gains = jnp.concatenate([gain_one.reshape(dp, rows), gain_two.reshape(dp, rows)], axis=1)
    gains = jnp.pad(gains, ((0, 0), (0, width - 2 * rows)))
    gains = jnp.tile(gains, (1, groups))[:, None]
    small = jnp.concatenate([maps, gains], axis=1).astype(bfloat)
    small = jnp.pad(small, ((0, 0), (0, 13), (0, 0)))
    full = [part.reshape(dp, -1, groups * width) for part in (up, down, square)]
    up, down, square, small = scatter_call(full + [small], dp, groups)
    return (
        small[2, :rows],
        small[2, rows : 2 * rows],
        small[:2].reshape(local, piece, size),
        square,
        up,
        down,
    )


def plain_gather(dp, groups, gain_one, gain_two, feature, square, up, down):
    def gathered(block):
        rows = lax.all_gather(block, "dp", axis=0, tiled=True)
        return lax.all_gather(rows, "tensor", axis=1, tiled=True)

    feature = lax.all_gather(feature, "dp", axis=1, tiled=True)
    return (
        lax.all_gather(gain_one, "dp", axis=0, tiled=True)[None],
        lax.all_gather(gain_two, "dp", axis=0, tiled=True)[None],
        lax.all_gather(feature, "tensor", axis=0, tiled=True),
        gathered(square),
        gathered(up),
        gathered(down),
    )


def plain_scatter(dp, groups, gain_one, gain_two, feature, square, up, down):
    def scattered(grad):
        rows = lax.psum_scatter(grad, "tensor", scatter_dimension=1, tiled=True)
        return lax.psum_scatter(rows, "dp", scatter_dimension=0, tiled=True).astype(single)

    feature = lax.psum_scatter(feature, "tensor", scatter_dimension=0, tiled=True)
    feature = lax.psum_scatter(feature, "dp", scatter_dimension=1, tiled=True)
    gains = lax.psum(jnp.concatenate([gain_one[0], gain_two[0]]), ("tensor", "dp"))
    rows = gain_one.shape[1] // dp
    place = lax.axis_index("dp") * rows
    return (
        lax.dynamic_slice(gains, (place,), (rows,)),
        lax.dynamic_slice(gains, (place + rows * dp,), (rows,)),
        feature,
        scattered(square),
        scattered(up),
        scattered(down),
    )


def per_device(
    groups, dp, tokens, gain_one, gain_two, qkv_weight, feature_weight, out_weight, up_weight,
    down_weight, cotangent,
):
    own = dp == 2 * LINE and groups == 4
    gather, scatter = (kernel_gather, kernel_scatter) if own else (plain_gather, plain_scatter)
    gain_first, gain_second, feature, square, up, down = gather(
        dp, groups,
        gain_one.astype(bfloat), gain_two.astype(bfloat), feature_weight.astype(bfloat),
        pack_square(qkv_weight.astype(bfloat), out_weight.astype(bfloat)),
        up_weight.astype(bfloat), down_weight.astype(bfloat).T,
    )
    (
        block_out, tokens_grad, gain_one_sum, gain_two_sum,
        square_grad, feature_grad, up_grad, down_grad,
    ) = compute(
        groups, tokens, cotangent, gain_first.astype(single), gain_second.astype(single),
        feature, square, up, down,
    )
    gain_one_out, gain_two_out, feature_out, square_out, up_out, down_out = scatter(
        dp, groups, gain_one_sum, gain_two_sum, feature_grad, square_grad, up_grad, down_grad
    )
    qkv_grad, out_grad = unpack_square(square_out)
    return (
        block_out, tokens_grad, gain_one_out, gain_two_out, qkv_grad, feature_out, out_grad,
        up_out, down_out.T,
    )


def solution(mesh):
    return jax.shard_map(
        functools.partial(per_device, mesh.shape["tensor"], mesh.shape["dp"]),
        mesh=mesh,
        in_specs=(
            P(("dp", "tensor"), None),
            P("dp"),
            P("dp"),
            P(None, "dp", "tensor"),
            P("tensor", "dp", None),
            P("tensor", "dp"),
            P("dp", "tensor"),
            P("tensor", "dp"),
            P(("dp", "tensor"), None),
        ),
        out_specs=(
            P(("dp", "tensor"), None),
            P(("dp", "tensor"), None),
            P("dp"),
            P("dp"),
            P(None, "dp", "tensor"),
            P("tensor", "dp", None),
            P("tensor", "dp"),
            P("dp", "tensor"),
            P("tensor", "dp"),
        ),
        check_vma=False,
    )
```
